256 devices in a mesh: farcp: 8 (over z), nearcp: 4 (over x), tp: 8 (over y, core).
Axes of the slice: x: 4, y: 4, z: 8, core: 2. Of those that a mesh axis runs over, the one named last changes fastest.
Arguments:
- raw_keys: bfloat16 [32, 16384, 8, 128], P(None, ('farcp', 'nearcp'), 'tp'), may hold values from -6 to 6
- raw_values: bfloat16 [32, 16384, 8, 128], P(None, ('farcp', 'nearcp'), 'tp'), may hold values from -6 to 6
- turn_angle: float32 [16384, 64], replicated, may hold values from -3.140625 to 3.140625
Outputs:
- stored_keys: bfloat16 [32, 16384, 8, 128], P(('farcp', 'nearcp'), None, 'tp')
- stored_values: bfloat16 [32, 16384, 8, 128], P(('farcp', 'nearcp'), None, 'tp')
- key_scale: float32 [32, 8, 128], P(('farcp', 'nearcp'), 'tp')
The draws below stay inside these ranges and needn't reach their ends.
All inputs are finite; a program needn't handle non-finite values. Where the reference program divides by a largest or mean magnitude, that divisor is 1e-20 or more.
Results may differ from the reference program's by a relative error of at most 0.001.
Values may be sent and summed in bfloat16 or wider, within the bound.
A program may use at most 128 MiB of HBM per device.

```python
import jax
import jax.numpy as jnp

BATCH = 32
LENGTH = 16384
KV_HEADS = 8
HEAD_SIZE = 128
HALF_HEAD = 64


def levels(own_key, shape, cuts, low, high):
    def one(axis_at, blocks):
        steps = jax.random.uniform(jax.random.fold_in(jax.random.fold_in(own_key, 6), axis_at), (blocks,), jnp.float32, low / len(cuts), high / len(cuts))
        return jnp.repeat(jnp.exp(steps), shape[axis_at] // blocks).reshape((-1,) + (1,) * (len(shape) - axis_at - 1))

    gain = one(*cuts[0])
    for cut in cuts[1:]:
        gain = gain * one(*cut)
    return gain


def noise(stream_key, extent, scale, bound, pieces=(), kind=jnp.bfloat16):
    result = jax.random.normal(stream_key, extent, jnp.float32) * scale
    if len(pieces) > 0:
        result = levels(stream_key, extent, pieces, -0.22, 0.18) * result
    return jnp.clip(result, min=-bound, max=bound).astype(kind)


def setup_inputs(seed: int = 0) -> dict:
    arg_keys = jax.random.split(jax.random.key(seed), 4)
    return {
        "raw_keys": noise(arg_keys[0], (BATCH, LENGTH, KV_HEADS, HEAD_SIZE), 1.0, 6.0, ((1, 32), (2, 8))),
        "raw_values": noise(arg_keys[1], (BATCH, LENGTH, KV_HEADS, HEAD_SIZE), 1.0, 6.0, ((1, 32), (2, 8))),
        "turn_angle": jnp.clip(jax.random.uniform(arg_keys[2], (LENGTH, HALF_HEAD), jnp.float32, -3.140625, 3.140625), -3.140625, 3.140625),
    }


def turn_pairs(vectors, angle):
    half = vectors.shape[-1] // 2
    cosine, sine = jnp.cos(angle)[None, :, None, :], jnp.sin(angle)[None, :, None, :]
    first, second = vectors[..., :half], vectors[..., half:]
    return jnp.concatenate([first * cosine - second * sine, second * cosine + first * sine], axis=-1)


def ready_to_store(plain_keys, angle):
    wide_keys = plain_keys.astype(jnp.float32)
    return turn_pairs(wide_keys, angle)


def reference(raw_keys, raw_values, turn_angle):
    turned_keys = ready_to_store(raw_keys, turn_angle)
    key_scale = jnp.max(jnp.abs(turned_keys), axis=1)
    narrow_keys = (turned_keys / key_scale[:, None]).astype(jnp.bfloat16)
    stored_keys = narrow_keys
    stored_values = raw_values
    return stored_keys, stored_values, key_scale
```

```python
import functools

import jax
import jax.numpy as jnp
from jax import lax
from jax.experimental import pallas as pl
from jax.experimental.pallas import tpu as pltpu
from jax.sharding import PartitionSpec as P

MESH = pl.DeviceIdType.MESH
AX = ("farcp", "nearcp")


def ring(d, n):
    return min(d % n, n - d % n)


def exchange(nf, nn, rows, half, keys, values, angle, narrow, moved, scale, landed, table_c, table_s, angles,
             key_send, key_recv, val_send, val_recv, own_sem, angle_sem):
    far, near = lax.axis_index("farcp"), lax.axis_index("nearcp")
    me = far * nn + near
    n = nf * nn
    steps = [(a, b) for a in range(nf) for b in range(nn) if (a, b) != (0, 0)]
    steps.sort(key=lambda s: (ring(s[0], nf), ring(s[1], nn)))

    def peer(step):
        return lax.rem(far + step[0], nf), lax.rem(near + step[1], nn)

    def block(index):
        return pl.ds(pl.multiple_of(index * rows, rows), rows)

    barrier = pltpu.get_barrier_semaphore()
    for step in steps:
        f, x = peer(step)
        pl.semaphore_signal(barrier, inc=1, device_id={"farcp": f, "nearcp": x}, device_id_type=MESH)
    own = [
        pltpu.make_async_copy(keys.at[me], landed.at[block(me)], own_sem.at[0]),
        pltpu.make_async_copy(values.at[me], moved.at[block(me)], own_sem.at[1]),
        pltpu.make_async_copy(angle, angles, angle_sem),
    ]
    for copy in own:
        copy.start()
    pl.semaphore_wait(barrier, n - 1)

    for source, target, send, recv in ((keys, landed, key_send, key_recv), (values, moved, val_send, val_recv)):
        for step in steps:
            f, x = peer(step)
            pltpu.make_async_remote_copy(
                source.at[f * nn + x], target.at[block(me)], send, recv,
                device_id={"farcp": f, "nearcp": x}, device_id_type=MESH,
            ).start()

    own[2].wait()

    def tables(i, carry):
        a = angles[:, block(i)]
        c, s = jnp.cos(a), jnp.sin(a)
        table_c[block(i), :] = jnp.concatenate([c, c], axis=0).T
        table_s[block(i), :] = jnp.concatenate([-s, s], axis=0).T
        return carry

    lax.fori_loop(0, n, tables, 0)

    def wait_all(ref, sem):
        part = ref.at[pl.ds(0, (n - 1) * rows)]
        pltpu.make_async_copy(part, part, sem).wait()

    own[0].wait()
    wait_all(landed, key_recv)

    def turn(i, largest):
        k = landed[block(i), :].astype(jnp.float32)
        t = k * table_c[block(i), :] + pltpu.roll(k, half, 1) * table_s[block(i), :]
        table_c[block(i), :] = t
        return jnp.maximum(largest, jnp.max(jnp.abs(t).reshape(rows // 8, 8, 2 * half), axis=0))

    largest = lax.fori_loop(0, n, turn, jnp.zeros((8, 2 * half), jnp.float32))
    top = jnp.max(largest, axis=0, keepdims=True)
    scale[...] = top

    def narrower(i, carry):
        narrow[block(i), :] = (table_c[block(i), :] / top).astype(jnp.bfloat16)
        return carry

    lax.fori_loop(0, n, narrower, 0)

    own[1].wait()
    wait_all(moved, val_recv)
    wait_all(landed, key_send)
    wait_all(moved, val_send)


def flush(narrow, moved, scale, narrow_out, moved_out, scale_out, sems):
    scale_out[...] = scale[...]
    n = 8
    rows = narrow.shape[0] // n
    copies = []
    for i in range(n):
        part = pl.ds(i * rows, rows)
        copies.append(pltpu.make_async_copy(narrow.at[part], narrow_out.at[part], sems.at[2 * i]))
        copies.append(pltpu.make_async_copy(moved.at[part], moved_out.at[part], sems.at[2 * i + 1]))
    for c in copies:
        c.start()
    for c in copies:
        c.wait()


def solution(mesh):
    nf, nn = mesh.shape["farcp"], mesh.shape["nearcp"]
    n = nf * nn

    def body(raw_keys, raw_values, turn_angle):
        batch, rows, _, size = raw_keys.shape
        length = rows * n
        keys = pltpu.with_memory_space_constraint(raw_keys.reshape(batch, rows, size), pltpu.HBM)
        values = pltpu.with_memory_space_constraint(raw_values.reshape(batch, rows, size), pltpu.HBM)
        angle = pltpu.with_memory_space_constraint(turn_angle.T, pltpu.HBM)
        wide = jax.ShapeDtypeStruct((length, size), jnp.bfloat16)
        small = jax.ShapeDtypeStruct((1, size), jnp.float32)
        hbm = pl.BlockSpec(memory_space=pltpu.HBM)
        vmem = pl.BlockSpec(memory_space=pltpu.VMEM)
        dma = pltpu.SemaphoreType.DMA
        narrow, moved, scale = pl.pallas_call(
            functools.partial(exchange, nf, nn, rows, size // 2),
            name="exchange",
            out_shape=(wide, wide, small),
            in_specs=[hbm] * 3,
            out_specs=(vmem, vmem, vmem),
            scratch_shapes=[
                pltpu.VMEM((length, size), jnp.bfloat16),
                pltpu.VMEM((length, size), jnp.float32),
                pltpu.VMEM((length, size), jnp.float32),
                pltpu.VMEM((size // 2, length), jnp.float32),
                dma, dma, dma, dma, dma((2,)), dma,
            ],
            compiler_params=pltpu.CompilerParams(
                collective_id=0, has_side_effects=True, vmem_limit_bytes=36 * 2**20
            ),
        )(keys, values, angle)
        stored_keys, stored_values, key_scale = pl.pallas_call(
            flush,
            name="flush",
            out_shape=(wide, wide, small),
            in_specs=[vmem, vmem, vmem],
            out_specs=(hbm, hbm, vmem),
            scratch_shapes=[dma((16,))],
            compiler_params=pltpu.CompilerParams(vmem_limit_bytes=4 * 2**20),
        )(narrow, moved, scale)
        return (
            stored_keys.reshape(1, length, 1, size),
            stored_values.reshape(1, length, 1, size),
            key_scale.reshape(1, 1, size),
        )

    return jax.shard_map(
        body, mesh=mesh,
        in_specs=(P(None, AX, "tp", None), P(None, AX, "tp", None), P()),
        out_specs=(P(AX, None, "tp", None), P(AX, None, "tp", None), P(AX, "tp", None)),
        check_vma=False,
    )
```

```python
import functools

import jax
import jax.numpy as jnp
from jax import lax
from jax.experimental import pallas as pl
from jax.experimental.pallas import tpu as pltpu
from jax.sharding import PartitionSpec as P

MESH = pl.DeviceIdType.MESH
AX = ("farcp", "nearcp")
PARTS = 2
NEXT = ((1, 0), (-1, 0), (0, 1), (0, -1))


def ring(d, n):
    return min(d % n, n - d % n)


def peers(nf, nn):
    pattern = [(1, 1), (-1, -1), (-1, 1), (1, -1), (1, 0), (-1, 0), (1, 2), (-1, 2)]
    order = [(sign * c % nf, b % nn) for c in [*range(1, nf // 2 + 1), 0] for sign, b in pattern]
    return [s for s in dict.fromkeys(order) if s != (0, 0)]


def exchange(nf, nn, rows, half, keys, values, angle, narrow, moved, scale, landed, table_c, table_s, angles,
             key_send, key_recv, val_send, val_recv, own_sem, angle_sem, entered):
    far, near = lax.axis_index("farcp"), lax.axis_index("nearcp")
    me = far * nn + near
    n = nf * nn
    steps = peers(nf, nn)

    def peer(step):
        return lax.rem(far + step[0] % nf, nf), lax.rem(near + step[1] % nn, nn)

    def block(index):
        return pl.ds(pl.multiple_of(index * rows, rows), rows)

    def start(source, target, send, recv, step, p):
        f, x = peer(step)
        here = pl.ds(pl.multiple_of(me * rows + p * part, part), part)
        pltpu.make_async_remote_copy(
            source.at[f * nn + x, pl.ds(p * part, part)], target.at[here], send, recv,
            device_id={"farcp": f, "nearcp": x}, device_id_type=MESH,
        ).start()

    barrier = pltpu.get_barrier_semaphore()
    for step in NEXT:
        f, x = peer(step)
        pl.semaphore_signal(barrier, inc=1, device_id={"farcp": f, "nearcp": x}, device_id_type=MESH)
    own = [
        pltpu.make_async_copy(keys.at[me], landed.at[block(me)], own_sem.at[0]),
        pltpu.make_async_copy(values.at[me], moved.at[block(me)], own_sem.at[1]),
        pltpu.make_async_copy(angle, angles, angle_sem),
    ]
    for copy in own:
        copy.start()
    pl.semaphore_wait(barrier, len(NEXT))

    part = rows // PARTS
    hops = nf // 2 + nn // 2
    for distance in range(1, hops + 1):
        if distance > 1:
            for i in range(len(NEXT)):
                pl.semaphore_wait(entered.at[i], 1)
        if distance < hops:
            for i, step in enumerate(NEXT):
                f, x = peer(step)
                pl.semaphore_signal(entered.at[i], inc=1, device_id={"farcp": f, "nearcp": x}, device_id_type=MESH)
        for step in steps:
            if ring(step[0], nf) + ring(step[1], nn) == distance:
                start(keys, landed, key_send, key_recv, step, 0)
    for p in range(1, PARTS):
        for step in steps:
            start(keys, landed, key_send, key_recv, step, p)
    for p in range(PARTS):
        for step in steps:
            start(values, moved, val_send, val_recv, step, p)

    own[2].wait()

    def tables(i, carry):
        a = angles[:, block(i)]
        c, s = jnp.cos(a), jnp.sin(a)
        table_c[block(i), :] = jnp.concatenate([c, c], axis=0).T
        table_s[block(i), :] = jnp.concatenate([-s, s], axis=0).T
        return carry

    lax.fori_loop(0, n, tables, 0)

    def wait_all(ref, sem):
        part = ref.at[pl.ds(0, (n - 1) * rows)]
        pltpu.make_async_copy(part, part, sem).wait()

    own[0].wait()
    wait_all(landed, key_recv)

    def turn(i, largest):
        k = landed[block(i), :].astype(jnp.float32)
        t = k * table_c[block(i), :] + pltpu.roll(k, half, 1) * table_s[block(i), :]
        table_c[block(i), :] = t
        return jnp.maximum(largest, jnp.max(jnp.abs(t).reshape(rows // 8, 8, 2 * half), axis=0))

    largest = lax.fori_loop(0, n, turn, jnp.zeros((8, 2 * half), jnp.float32))
    top = jnp.max(largest, axis=0, keepdims=True)
    scale[...] = top

    def narrower(i, carry):
        narrow[block(i), :] = (table_c[block(i), :] / top).astype(jnp.bfloat16)
        return carry

    lax.fori_loop(0, n, narrower, 0)

    own[1].wait()
    wait_all(moved, val_recv)
    wait_all(landed, key_send)
    wait_all(moved, val_send)


def flush(narrow, moved, scale, narrow_out, moved_out, scale_out, sems):
    pieces = 8
    rows = narrow.shape[0] // pieces
    copies = [pltpu.make_async_copy(scale, scale_out, sems.at[2 * pieces])]
    for i in range(pieces):
        part = pl.ds(i * rows, rows)
        copies.append(pltpu.make_async_copy(narrow.at[part], narrow_out.at[part], sems.at[2 * i]))
        copies.append(pltpu.make_async_copy(moved.at[part], moved_out.at[part], sems.at[2 * i + 1]))
    for copy in copies:
        copy.start()
    for copy in copies:
        copy.wait()


def solution(mesh):
    nf, nn = mesh.shape["farcp"], mesh.shape["nearcp"]
    n = nf * nn

    def body(raw_keys, raw_values, turn_angle):
        batch, rows, _, size = raw_keys.shape
        length = rows * n
        keys = pltpu.with_memory_space_constraint(raw_keys.reshape(batch, rows, size), pltpu.HBM)
        values = pltpu.with_memory_space_constraint(raw_values.reshape(batch, rows, size), pltpu.HBM)
        angle = pltpu.with_memory_space_constraint(turn_angle.T, pltpu.HBM)
        wide = jax.ShapeDtypeStruct((length, size), jnp.bfloat16)
        small = jax.ShapeDtypeStruct((1, size), jnp.float32)
        hbm = pl.BlockSpec(memory_space=pltpu.HBM)
        vmem = pl.BlockSpec(memory_space=pltpu.VMEM)
        dma = pltpu.SemaphoreType.DMA
        narrow, moved, scale = pl.pallas_call(
            functools.partial(exchange, nf, nn, rows, size // 2),
            name="exchange",
            out_shape=(wide, wide, small),
            in_specs=[hbm] * 3,
            out_specs=(vmem, vmem, vmem),
            scratch_shapes=[
                pltpu.VMEM((length, size), jnp.bfloat16),
                pltpu.VMEM((length, size), jnp.float32),
                pltpu.VMEM((length, size), jnp.float32),
                pltpu.VMEM((size // 2, length), jnp.float32),
                dma, dma, dma, dma, dma((2,)), dma,
                pltpu.SemaphoreType.REGULAR((len(NEXT),)),
            ],
            compiler_params=pltpu.CompilerParams(
                collective_id=0, has_side_effects=True, vmem_limit_bytes=36 * 2**20
            ),
        )(keys, values, angle)
        stored_keys, stored_values, key_scale = pl.pallas_call(
            flush,
            name="flush",
            out_shape=(wide, wide, small),
            in_specs=[vmem, vmem, vmem],
            out_specs=(hbm, hbm, hbm),
            scratch_shapes=[dma((17,))],
            compiler_params=pltpu.CompilerParams(vmem_limit_bytes=4 * 2**20),
        )(narrow, moved, scale)
        return (
            stored_keys.reshape(1, length, 1, size),
            stored_values.reshape(1, length, 1, size),
            key_scale.reshape(1, 1, size),
        )

    return jax.shard_map(
        body, mesh=mesh,
        in_specs=(P(None, AX, "tp", None), P(None, AX, "tp", None), P()),
        out_specs=(P(AX, None, "tp", None), P(AX, None, "tp", None), P(AX, "tp", None)),
        check_vma=False,
    )
```

```python
import functools

import jax
import jax.numpy as jnp
from jax import lax
from jax.experimental import pallas as pl
from jax.experimental.pallas import tpu as pltpu
from jax.sharding import PartitionSpec as P

MESH = pl.DeviceIdType.MESH
AX = ("farcp", "nearcp")
NEXT = ((1, 0), (-1, 0), (0, 1), (0, -1))
PASSES = 4


def ring(d, n):
    return min(d % n, n - d % n)


def peers(nf, nn):
    pattern = [(1, 1), (-1, -1), (-1, 1), (1, -1), (1, 0), (-1, 0), (1, 2), (-1, 2)]
    order = [(sign * c % nf, b % nn) for c in [*range(1, nf // 2 + 1), 0] for sign, b in pattern]
    return [s for s in dict.fromkeys(order) if s != (0, 0)]


def deadlines(nf, nn):
    far = [*range(nf // 2), nf - 1, *range(nf // 2, nf - 1)]
    near = [*range(nn - 2), nn - 1, nn - 2]
    return [(f, x) for f in far for x in near]


def exchange(nf, nn, rows, half, keys, values, angle, narrow, moved, scale, landed, table_c, table_s, angles, first,
             key_send, key_recv, val_send, val_recv, own_sem, angle_sem, first_sem, entered):
    far, near = lax.axis_index("farcp"), lax.axis_index("nearcp")
    me = far * nn + near
    n = nf * nn
    steps = peers(nf, nn)
    middle = rows // 2

    def peer(step):
        return lax.rem(far + step[0] % nf, nf), lax.rem(near + step[1] % nn, nn)

    def block(index):
        return pl.ds(pl.multiple_of(index * rows, rows), rows)

    def push(source, target, send, recv, f, x):
        pltpu.make_async_remote_copy(
            source, target, send, recv, device_id={"farcp": f, "nearcp": x}, device_id_type=MESH
        ).start()

    def here(at, size):
        return pl.ds(pl.multiple_of(me * rows + at, size), size)

    def push_keys(f, x, at, size):
        push(keys.at[f * nn + x, pl.ds(at, size)], landed.at[here(at, size)], key_send, key_recv, f, x)

    def push_values(f, x, at, size):
        push(values.at[f * nn + x, pl.ds(at, size)], moved.at[here(at, size)], val_send, val_recv, f, x)

    barrier = pltpu.get_barrier_semaphore()
    for step in NEXT:
        f, x = peer(step)
        pl.semaphore_signal(barrier, inc=1, device_id={"farcp": f, "nearcp": x}, device_id_type=MESH)
    early = []
    for i, step in enumerate(NEXT):
        f, x = peer(step)
        early.append(pltpu.make_async_copy(keys.at[f * nn + x], first.at[i], first_sem.at[i]))
    own = [
        pltpu.make_async_copy(keys.at[me], landed.at[block(me)], own_sem.at[0]),
        pltpu.make_async_copy(values.at[me], moved.at[block(me)], own_sem.at[1]),
        pltpu.make_async_copy(angle, angles, angle_sem),
    ]
    for copy in early + own:
        copy.start()
    pl.semaphore_wait(barrier, len(NEXT))
    for i, step in enumerate(NEXT):
        early[i].wait()
        push(first.at[i], landed.at[block(me)], key_send, key_recv, *peer(step))

    for distance in range(2, nf // 2 + nn // 2 + 1):
        for i, step in enumerate(NEXT):
            f, x = peer(step)
            pl.semaphore_signal(entered.at[i], inc=1, device_id={"farcp": f, "nearcp": x}, device_id_type=MESH)
        for i in range(len(NEXT)):
            pl.semaphore_wait(entered.at[i], 1)
        for step in steps:
            if ring(step[0], nf) + ring(step[1], nn) == distance:
                push_keys(*peer(step), 0, middle)

    for step in steps:
        if ring(step[0], nf) + ring(step[1], nn) > 1:
            push_keys(*peer(step), middle, middle)
    for step in steps:
        push_values(*peer(step), 0, middle)
    size = middle // PASSES
    for p in range(PASSES):
        for f, x in deadlines(nf, nn):
            pl.when((far != f) | (near != x))(functools.partial(push_values, f, x, middle + p * size, size))

    own[2].wait()

    def tables(i, carry):
        a = angles[:, block(i)]
        c, s = jnp.cos(a), jnp.sin(a)
        table_c[block(i), :] = jnp.concatenate([c, c], axis=0).T
        table_s[block(i), :] = jnp.concatenate([-s, s], axis=0).T
        return carry

    lax.fori_loop(0, n, tables, 0)

    def wait_all(ref, sem):
        part = ref.at[pl.ds(0, (n - 1) * rows)]
        pltpu.make_async_copy(part, part, sem).wait()

    own[0].wait()
    wait_all(landed, key_recv)

    def turn(i, largest):
        k = landed[block(i), :].astype(jnp.float32)
        t = k * table_c[block(i), :] + pltpu.roll(k, half, 1) * table_s[block(i), :]
        table_c[block(i), :] = t
        return jnp.maximum(largest, jnp.max(jnp.abs(t).reshape(rows // 8, 8, 2 * half), axis=0))

    largest = lax.fori_loop(0, n, turn, jnp.zeros((8, 2 * half), jnp.float32))
    top = jnp.max(largest, axis=0, keepdims=True)
    scale[...] = top

    def narrower(i, carry):
        narrow[block(i), :] = (table_c[block(i), :] / top).astype(jnp.bfloat16)
        return carry

    lax.fori_loop(0, n, narrower, 0)

    own[1].wait()
    wait_all(moved, val_recv)
    wait_all(landed, key_send)
    wait_all(moved, val_send)


def flush(narrow, moved, scale, narrow_out, moved_out, scale_out, sems):
    pieces = 4
    rows = narrow.shape[0] // pieces
    copies = [pltpu.make_async_copy(scale, scale_out, sems.at[2 * pieces])]
    for i in range(pieces):
        part = pl.ds(i * rows, rows)
        copies.append(pltpu.make_async_copy(narrow.at[part], narrow_out.at[part], sems.at[2 * i]))
        copies.append(pltpu.make_async_copy(moved.at[part], moved_out.at[part], sems.at[2 * i + 1]))
    for copy in copies:
        copy.start()
    for copy in copies:
        copy.wait()


def solution(mesh):
    nf, nn = mesh.shape["farcp"], mesh.shape["nearcp"]
    n = nf * nn

    def body(raw_keys, raw_values, turn_angle):
        batch, rows, _, size = raw_keys.shape
        length = rows * n
        keys, values, angle = (
            pltpu.with_memory_space_constraint(a, pltpu.HBM)
            for a in (raw_keys.reshape(batch, rows, size), raw_values.reshape(batch, rows, size), turn_angle.T)
        )
        wide = jax.ShapeDtypeStruct((length, size), jnp.bfloat16)
        small = jax.ShapeDtypeStruct((1, size), jnp.float32)
        hbm = pl.BlockSpec(memory_space=pltpu.HBM)
        vmem = pl.BlockSpec(memory_space=pltpu.VMEM)
        dma = pltpu.SemaphoreType.DMA
        narrow, moved, scale = pl.pallas_call(
            functools.partial(exchange, nf, nn, rows, size // 2),
            name="exchange",
            out_shape=(wide, wide, small),
            in_specs=[hbm] * 3,
            out_specs=(vmem, vmem, vmem),
            scratch_shapes=[
                pltpu.VMEM((length, size), jnp.bfloat16),
                pltpu.VMEM((length, size), jnp.float32),
                pltpu.VMEM((length, size), jnp.float32),
                pltpu.VMEM((size // 2, length), jnp.float32),
                pltpu.VMEM((len(NEXT), rows, size), jnp.bfloat16),
                dma, dma, dma, dma, dma((2,)), dma, dma((len(NEXT),)),
                pltpu.SemaphoreType.REGULAR((len(NEXT),)),
            ],
            compiler_params=pltpu.CompilerParams(
                collective_id=0, has_side_effects=True, vmem_limit_bytes=36 * 2**20
            ),
        )(keys, values, angle)
        stored_keys, stored_values, key_scale = pl.pallas_call(
            flush,
            name="flush",
            out_shape=(wide, wide, small),
            in_specs=[vmem, vmem, vmem],
            out_specs=(hbm, hbm, hbm),
            scratch_shapes=[dma((9,))],
            compiler_params=pltpu.CompilerParams(vmem_limit_bytes=4 * 2**20),
        )(narrow, moved, scale)
        return (
            stored_keys.reshape(1, length, 1, size),
            stored_values.reshape(1, length, 1, size),
            key_scale.reshape(1, 1, size),
        )

    return jax.shard_map(
        body, mesh=mesh,
        in_specs=(P(None, AX, "tp", None), P(None, AX, "tp", None), P()),
        out_specs=(P(AX, None, "tp", None), P(AX, None, "tp", None), P(AX, "tp", None)),
        check_vma=False,
    )
```

```python
import functools

import jax
import jax.numpy as jnp
from jax import lax
from jax.experimental import pallas as pl
from jax.experimental.pallas import tpu as pltpu
from jax.sharding import PartitionSpec as P

MESH = pl.DeviceIdType.MESH
AX = ("farcp", "nearcp")
NEXT = ((1, 0), (-1, 0), (0, 1), (0, -1))
PASSES = ((1, 2), (2, 4))


def ring(d, n):
    return min(d % n, n - d % n)


def peers(nf, nn):
    pattern = [(1, 1), (-1, -1), (-1, 1), (1, -1), (1, 0), (-1, 0), (1, 2), (-1, 2)]
    order = [(sign * c % nf, b % nn) for c in [*range(1, nf // 2 + 1), 0] for sign, b in pattern]
    return [s for s in dict.fromkeys(order) if s != (0, 0)]


def deadlines(nf, nn):
    far = [*range(nf // 2), nf - 1, *range(nf // 2, nf - 1)]
    near = [*range(nn - 2), nn - 1, nn - 2]
    return [(f, x) for f in far for x in near]


def exchange(nf, nn, rows, half, keys, values, angle, narrow, moved, scale, landed, table_c, table_s, angles, first,
             key_send, key_recv, val_send, val_recv, own_sem, angle_sem, first_sem, entered):
    far, near = lax.axis_index("farcp"), lax.axis_index("nearcp")
    me = far * nn + near
    n = nf * nn
    steps = peers(nf, nn)
    middle = rows // 2

    def peer(step):
        return lax.rem(far + step[0] % nf, nf), lax.rem(near + step[1] % nn, nn)

    def block(index):
        return pl.ds(pl.multiple_of(index * rows, rows), rows)

    def push(source, target, send, recv, f, x):
        pltpu.make_async_remote_copy(
            source, target, send, recv, device_id={"farcp": f, "nearcp": x}, device_id_type=MESH
        ).start()

    def here(at, size):
        return pl.ds(pl.multiple_of(me * rows + at, size), size)

    def push_keys(f, x, at, size):
        push(keys.at[f * nn + x, pl.ds(at, size)], landed.at[here(at, size)], key_send, key_recv, f, x)

    def push_values(f, x, at, size):
        push(values.at[f * nn + x, pl.ds(at, size)], moved.at[here(at, size)], val_send, val_recv, f, x)

    barrier = pltpu.get_barrier_semaphore()
    for step in NEXT:
        f, x = peer(step)
        pl.semaphore_signal(barrier, inc=1, device_id={"farcp": f, "nearcp": x}, device_id_type=MESH)
    early = []
    for i, step in enumerate(NEXT):
        f, x = peer(step)
        early.append(pltpu.make_async_copy(keys.at[f * nn + x], first.at[i], first_sem.at[i]))
    own = [
        pltpu.make_async_copy(keys.at[me], landed.at[block(me)], own_sem.at[0]),
        pltpu.make_async_copy(values.at[me], moved.at[block(me)], own_sem.at[1]),
        pltpu.make_async_copy(angle, angles, angle_sem),
    ]
    for copy in early + own:
        copy.start()
    pl.semaphore_wait(barrier, len(NEXT))
    for i, step in enumerate(NEXT):
        early[i].wait()
        push(first.at[i], landed.at[block(me)], key_send, key_recv, *peer(step))

    for distance in range(2, nf // 2 + nn // 2 + 1):
        for i, step in enumerate(NEXT):
            f, x = peer(step)
            pl.semaphore_signal(entered.at[i], inc=1, device_id={"farcp": f, "nearcp": x}, device_id_type=MESH)
        for i in range(len(NEXT)):
            pl.semaphore_wait(entered.at[i], 1)
        for step in steps:
            if ring(step[0], nf) + ring(step[1], nn) == distance:
                push_keys(*peer(step), 0, middle)

    for step in steps:
        if ring(step[0], nf) + ring(step[1], nn) > 1:
            push_keys(*peer(step), middle, middle)
    def all_values(passes):
        at = 0
        for size in passes:
            for f, x in deadlines(nf, nn):
                pl.when((far != f) | (near != x))(functools.partial(push_values, f, x, at, size))
            at += size

    for core, passes in enumerate(PASSES):
        sizes = [middle // p for p in passes for _ in range(p)]
        pl.when(lax.rem(lax.axis_index("tp"), 2) == core)(functools.partial(all_values, sizes))

    own[2].wait()

    def tables(i, carry):
        a = angles[:, block(i)]
        c, s = jnp.cos(a), jnp.sin(a)
        table_c[block(i), :] = jnp.concatenate([c, c], axis=0).T
        table_s[block(i), :] = jnp.concatenate([-s, s], axis=0).T
        return carry

    lax.fori_loop(0, n, tables, 0)

    def wait_all(ref, sem):
        part = ref.at[pl.ds(0, (n - 1) * rows)]
        pltpu.make_async_copy(part, part, sem).wait()

    own[0].wait()
    wait_all(landed, key_recv)

    def turn(i, largest):
        k = landed[block(i), :].astype(jnp.float32)
        t = k * table_c[block(i), :] + pltpu.roll(k, half, 1) * table_s[block(i), :]
        table_c[block(i), :] = t
        return jnp.maximum(largest, jnp.max(jnp.abs(t).reshape(rows // 8, 8, 2 * half), axis=0))

    largest = lax.fori_loop(0, n, turn, jnp.zeros((8, 2 * half), jnp.float32))
    top = jnp.max(largest, axis=0, keepdims=True)
    scale[...] = top

    def narrower(i, carry):
        narrow[block(i), :] = (table_c[block(i), :] / top).astype(jnp.bfloat16)
        return carry

    lax.fori_loop(0, n, narrower, 0)

    own[1].wait()
    wait_all(moved, val_recv)
    wait_all(landed, key_send)
    wait_all(moved, val_send)


def flush(narrow, moved, scale, narrow_out, moved_out, scale_out, sems):
    pieces = 4
    rows = narrow.shape[0] // pieces
    copies = [pltpu.make_async_copy(scale, scale_out, sems.at[2 * pieces])]
    for i in range(pieces):
        part = pl.ds(i * rows, rows)
        copies.append(pltpu.make_async_copy(narrow.at[part], narrow_out.at[part], sems.at[2 * i]))
        copies.append(pltpu.make_async_copy(moved.at[part], moved_out.at[part], sems.at[2 * i + 1]))
    for copy in copies:
        copy.start()
    for copy in copies:
        copy.wait()


def solution(mesh):
    nf, nn = mesh.shape["farcp"], mesh.shape["nearcp"]
    n = nf * nn

    def body(raw_keys, raw_values, turn_angle):
        batch, rows, _, size = raw_keys.shape
        length = rows * n
        keys, values, angle = (
            pltpu.with_memory_space_constraint(a, pltpu.HBM)
            for a in (raw_keys.reshape(batch, rows, size), raw_values.reshape(batch, rows, size), turn_angle.T)
        )
        wide = jax.ShapeDtypeStruct((length, size), jnp.bfloat16)
        small = jax.ShapeDtypeStruct((1, size), jnp.float32)
        hbm = pl.BlockSpec(memory_space=pltpu.HBM)
        vmem = pl.BlockSpec(memory_space=pltpu.VMEM)
        dma = pltpu.SemaphoreType.DMA
        narrow, moved, scale = pl.pallas_call(
            functools.partial(exchange, nf, nn, rows, size // 2),
            name="exchange",
            out_shape=(wide, wide, small),
            in_specs=[hbm] * 3,
            out_specs=(vmem, vmem, vmem),
            scratch_shapes=[
                pltpu.VMEM((length, size), jnp.bfloat16),
                pltpu.VMEM((length, size), jnp.float32),
                pltpu.VMEM((length, size), jnp.float32),
                pltpu.VMEM((size // 2, length), jnp.float32),
                pltpu.VMEM((len(NEXT), rows, size), jnp.bfloat16),
                dma, dma, dma, dma, dma((2,)), dma, dma((len(NEXT),)),
                pltpu.SemaphoreType.REGULAR((len(NEXT),)),
            ],
            compiler_params=pltpu.CompilerParams(
                collective_id=0, has_side_effects=True, vmem_limit_bytes=36 * 2**20
            ),
        )(keys, values, angle)
        stored_keys, stored_values, key_scale = pl.pallas_call(
            flush,
            name="flush",
            out_shape=(wide, wide, small),
            in_specs=[vmem, vmem, vmem],
            out_specs=(hbm, hbm, hbm),
            scratch_shapes=[dma((9,))],
            compiler_params=pltpu.CompilerParams(vmem_limit_bytes=4 * 2**20),
        )(narrow, moved, scale)
        return (
            stored_keys.reshape(1, length, 1, size),
            stored_values.reshape(1, length, 1, size),
            key_scale.reshape(1, 1, size),
        )

    return jax.shard_map(
        body, mesh=mesh,
        in_specs=(P(None, AX, "tp", None), P(None, AX, "tp", None), P()),
        out_specs=(P(AX, None, "tp", None), P(AX, None, "tp", None), P(AX, "tp", None)),
        check_vma=False,
    )
```
